32 devices in a mesh: dp: 4 (over x, core), pipe: 2 (over y), tensor: 4 (over z).
Axes of the slice: x: 2, y: 2, z: 4, core: 2. Of those that a mesh axis runs over, the one named last changes fastest.
Arguments:
- weights: bfloat16 [2816, 1408], P(('dp', 'pipe', 'tensor')), may hold values from -6 to 6
- first_moment: bfloat16 [2816, 1408], P(('dp', 'pipe', 'tensor')), may hold values from -6 to 6
- second_moment: bfloat16 [2816, 1408], P(('dp', 'pipe', 'tensor')), may hold values from 0.049804688 to 5
- row_weight: float32 [1408], replicated, may hold values from -1 to 1
- col_weight: float32 [1408], replicated, may hold values from 1 to 4
Outputs:
- weight_tiles: bfloat16 [2816, 1408], P(('pipe', 'tensor'))
- first_tiles: bfloat16 [2816, 1408], P(('pipe', 'tensor'))
- second_tiles: bfloat16 [2816, 1408], P(('pipe', 'tensor'))
- checksums: float32 [3, 2, 4, 11], P(None, 'pipe', 'tensor')
The draws below stay inside these ranges and needn't reach their ends.
All inputs are finite; a program needn't handle non-finite values.
Results may differ from the reference program's by a relative error of at most 0.001.
Values may be sent and summed in bfloat16 or wider, within the bound.
A program may use at most 64 MiB of HBM per device.

```python
import math
import jax
import jax.numpy as jnp
from jax import lax

D = 1408
CHECK_COLS = 128
BLOCKS = 2
N_TENSOR = 4


def block_scale(key, dims, shards, low, high):
    gain = 1.0
    for position, blocks in shards:
        heights = jax.random.uniform(jax.random.fold_in(jax.random.fold_in(key, 6), position), (blocks,), jnp.float32, low / len(shards), high / len(shards))
        gain = gain * jnp.repeat(jnp.exp(heights), dims[position] // blocks).reshape((-1,) + (1,) * (len(dims) - 1 - position))
    return gain


def scatter_about(stream_key, dims, width, bound, pieces=(), kind=jnp.bfloat16):
    values = width * jax.random.normal(stream_key, dims, jnp.float32)
    if pieces:
        values = values * block_scale(stream_key, dims, pieces, -0.22, 0.18)
    return jnp.clip(values, -bound, bound).astype(kind)


def setup_inputs(seed: int = 0) -> dict:
    seeds = jax.random.split(jax.random.key(seed), 6)
    return {
        "weights": scatter_about(seeds[0], (BLOCKS * D, D), 1.0, 6.0, ((0, 32),)),
        "first_moment": scatter_about(seeds[1], (BLOCKS * D, D), 1.0, 6.0, ((0, 32),)),
        "second_moment": jnp.clip(jnp.exp(math.log(5.0) - 4.609084 * jax.random.uniform(seeds[2], (BLOCKS * D, D), jnp.float32) ** block_scale(seeds[2], (BLOCKS * D, D), ((0, 32),), -0.2, 0.2)), 0.049804688, 5.0).astype(jnp.bfloat16),
        "row_weight": jnp.clip(jax.random.uniform(seeds[3], (D,), jnp.float32, -1.0, 1.0), -1.0, 1.0),
        "col_weight": jnp.clip(jnp.exp(jax.random.uniform(seeds[4], (D,), jnp.float32, math.log(1.0), math.log(4.0))), 1.0, 4.0),
    }


def reference(weights, first_moment, second_moment, row_weight, col_weight):
    tile_rows = D // N_TENSOR
    col_blocks = D // CHECK_COLS
    factor = float(tile_rows * CHECK_COLS) ** -0.5
    row_grid = row_weight.reshape(N_TENSOR, tile_rows)
    col_grid = col_weight.reshape(col_blocks, CHECK_COLS)

    def one_kind(data):
        blocked = data.astype(jnp.float32).reshape(BLOCKS, N_TENSOR, tile_rows, col_blocks, CHECK_COLS)
        weighted = jnp.einsum("bjrce,jr->bjce", blocked, row_grid, precision=lax.Precision.HIGHEST)
        return factor * jnp.sum(weighted * col_grid, axis=3)

    checks = jnp.stack([one_kind(weights), one_kind(first_moment), one_kind(second_moment)]).astype(jnp.float32)
    return weights, first_moment, second_moment, checks
```

```python
import functools

import jax
import jax.numpy as jnp
from jax import lax
from jax.experimental import pallas as pl
from jax.experimental.pallas import tpu as pltpu
from jax.sharding import PartitionSpec as P

CHECK_COLS = 128
SPLIT = 4
OWN_UNITS, OFF_UNITS = 8, 7
ORDER = {
    (True, True, 0): (
        (0, 0, 0), (0, 0, 1), (0, 0, 2), (0, 0, 3), (0, 0, 4), (0, 0, 5), (0, 0, 6), (0, 0, 7),
        (0, 3, 0), (0, 3, 1), (0, 3, 2), (0, 3, 3), (0, 3, 4), (0, 3, 5), (0, 3, 6), (0, 1, 0),
        (0, 3, 7), (0, 2, 0), (0, 1, 1), (0, 2, 1), (0, 1, 2), (0, 2, 2), (0, 1, 3), (0, 2, 3),
        (0, 1, 4), (0, 2, 4), (0, 1, 5), (0, 2, 5), (0, 1, 6), (0, 2, 6), (0, 1, 7), (0, 2, 7),
    ),
    (True, True, 1): (
        (0, 1, 0), (0, 1, 1), (0, 1, 2), (0, 1, 3), (0, 0, 0), (0, 1, 4), (0, 0, 1), (0, 3, 0),
        (0, 1, 5), (0, 0, 2), (0, 3, 1), (0, 1, 6), (0, 0, 3), (0, 3, 2), (0, 0, 4), (0, 3, 3),
        (0, 0, 5), (0, 3, 4), (0, 0, 6), (0, 3, 5), (0, 3, 6), (0, 2, 0), (0, 2, 1), (0, 2, 2),
        (0, 2, 3), (0, 2, 4), (0, 2, 5), (0, 2, 6),
    ),
    (True, True, 2): (
        (0, 2, 0), (0, 2, 1), (0, 2, 2), (0, 2, 3), (0, 2, 4), (0, 2, 5), (0, 2, 6), (0, 2, 7),
        (0, 0, 0), (0, 0, 1), (0, 0, 2), (0, 0, 3), (0, 0, 4), (0, 0, 5), (0, 0, 6), (0, 1, 0),
        (0, 0, 7), (0, 3, 0), (0, 1, 1), (0, 3, 1), (0, 1, 2), (0, 3, 2), (0, 1, 3), (0, 3, 3),
        (0, 1, 4), (0, 3, 4), (0, 1, 5), (0, 3, 5), (0, 1, 6), (0, 3, 6), (0, 1, 7), (0, 3, 7),
    ),
    (True, True, 3): (
        (0, 3, 0), (0, 3, 1), (0, 2, 0), (0, 3, 2), (0, 2, 1), (0, 3, 3), (0, 3, 4), (0, 2, 2),
        (0, 3, 5), (0, 0, 0), (0, 2, 3), (0, 3, 6), (0, 0, 1), (0, 2, 4), (0, 0, 2), (0, 2, 5),
        (0, 0, 3), (0, 2, 6), (0, 0, 4), (0, 0, 5), (0, 0, 6), (0, 1, 0), (0, 1, 1), (0, 1, 2),
        (0, 1, 3), (0, 1, 4), (0, 1, 5), (0, 1, 6),
    ),
    (True, False, 0): (
        (1, 0, 0), (1, 1, 0), (1, 0, 1), (1, 1, 1), (1, 0, 2), (1, 1, 2), (1, 0, 3), (1, 1, 3),
        (1, 0, 4), (1, 1, 4), (1, 0, 5), (1, 1, 5), (1, 0, 6), (1, 1, 6), (0, 1, 8), (0, 3, 8),
        (0, 1, 9), (0, 3, 9), (0, 1, 10), (0, 3, 10), (0, 1, 11), (0, 3, 11), (0, 0, 8), (0, 0, 9),
        (0, 0, 10), (0, 2, 8), (0, 0, 11), (0, 2, 9), (0, 2, 10), (0, 2, 11),
    ),
    (True, False, 1): (
        (1, 1, 0), (1, 1, 1), (1, 1, 2), (1, 1, 3), (1, 1, 4), (1, 1, 5), (1, 1, 6), (0, 1, 7),
        (0, 1, 8), (0, 1, 9), (0, 1, 10), (0, 1, 11), (0, 3, 7), (0, 3, 8), (0, 3, 9), (0, 3, 10),
        (0, 0, 7), (0, 3, 11), (0, 2, 7), (0, 0, 8), (0, 0, 9), (0, 2, 8), (0, 0, 10), (0, 0, 11),
        (0, 2, 9), (0, 2, 10), (0, 2, 11),
    ),
    (True, False, 2): (
        (1, 0, 0), (1, 1, 0), (1, 0, 1), (1, 1, 1), (1, 0, 2), (1, 1, 2), (1, 0, 3), (1, 1, 3),
        (1, 0, 4), (1, 1, 4), (1, 0, 5), (1, 1, 5), (1, 0, 6), (1, 1, 6), (0, 3, 8), (0, 3, 9),
        (0, 1, 8), (0, 3, 10), (0, 1, 9), (0, 1, 10), (0, 3, 11), (0, 1, 11), (0, 2, 8), (0, 2, 9),
        (0, 2, 10), (0, 0, 8), (0, 2, 11), (0, 0, 9), (0, 0, 10), (0, 0, 11),
    ),
    (True, False, 3): (
        (1, 0, 0), (1, 0, 1), (1, 0, 2), (1, 0, 3), (1, 0, 4), (1, 0, 5), (1, 0, 6), (0, 3, 7),
        (0, 3, 8), (0, 3, 9), (0, 3, 10), (0, 3, 11), (0, 0, 7), (0, 0, 8), (0, 0, 9), (0, 0, 10),
        (0, 1, 7), (0, 0, 11), (0, 1, 8), (0, 1, 9), (0, 1, 10), (0, 2, 7), (0, 1, 11), (0, 2, 8),
        (0, 2, 9), (0, 2, 10), (0, 2, 11),
    ),
    (False, True, 0): (
        (0, 1, 8), (0, 3, 8), (0, 1, 9), (0, 3, 9), (0, 1, 10), (0, 3, 10), (0, 1, 11), (0, 3, 11),
        (0, 0, 8), (0, 0, 9), (0, 0, 10), (0, 2, 8), (0, 0, 11), (0, 2, 9), (0, 2, 10), (0, 2, 11),
    ),
    (False, True, 1): (
        (0, 1, 7), (0, 1, 8), (0, 1, 9), (0, 1, 10), (0, 1, 11), (0, 3, 7), (0, 3, 8), (0, 3, 9),
        (0, 3, 10), (0, 0, 7), (0, 3, 11), (0, 0, 8), (0, 2, 7), (0, 0, 9), (0, 0, 10), (0, 2, 8),
        (0, 0, 11), (0, 2, 9), (0, 2, 10), (0, 2, 11),
    ),
    (False, True, 2): (
        (0, 3, 8), (0, 3, 9), (0, 1, 8), (0, 3, 10), (0, 1, 9), (0, 1, 10), (0, 3, 11), (0, 1, 11),
        (0, 2, 8), (0, 2, 9), (0, 2, 10), (0, 0, 8), (0, 2, 11), (0, 0, 9), (0, 0, 10), (0, 0, 11),
    ),
    (False, True, 3): (
        (0, 3, 7), (0, 3, 8), (0, 3, 9), (0, 3, 10), (0, 3, 11), (0, 0, 7), (0, 0, 8), (0, 0, 9),
        (0, 0, 10), (0, 1, 7), (0, 0, 11), (0, 1, 8), (0, 1, 9), (0, 1, 10), (0, 2, 7), (0, 1, 11),
        (0, 2, 8), (0, 2, 9), (0, 2, 10), (0, 2, 11),
    ),
    (False, False, 0): (
        (1, 1, 8), (1, 1, 9), (1, 1, 10), (1, 1, 11), (0, 0, 7), (0, 0, 8), (0, 0, 9), (0, 0, 0),
        (0, 0, 10), (0, 0, 11), (0, 0, 1), (0, 3, 7), (0, 1, 0), (0, 3, 8), (0, 0, 2), (0, 3, 9),
        (0, 1, 1), (0, 3, 10), (0, 0, 3), (0, 2, 7), (0, 3, 11), (0, 1, 2), (0, 2, 8), (0, 0, 4),
        (0, 2, 9), (0, 3, 0), (0, 2, 10), (0, 1, 3), (0, 1, 7), (0, 0, 5), (0, 2, 11), (0, 3, 1),
        (0, 1, 8), (0, 1, 4), (0, 1, 9), (0, 0, 6), (0, 1, 10), (0, 3, 2), (0, 1, 11), (0, 1, 5),
        (0, 3, 3), (0, 1, 6), (0, 3, 4), (0, 3, 5), (0, 3, 6), (0, 2, 0), (0, 2, 1), (0, 2, 2),
        (0, 2, 3), (0, 2, 4), (0, 2, 5), (0, 2, 6),
    ),
    (False, False, 1): (
        (1, 0, 8), (1, 1, 8), (1, 0, 9), (1, 1, 9), (1, 0, 10), (1, 1, 10), (1, 0, 11), (1, 1, 11),
        (0, 1, 0), (0, 1, 1), (0, 1, 2), (0, 1, 3), (0, 1, 4), (0, 1, 5), (0, 1, 6), (0, 1, 7),
        (0, 3, 0), (0, 0, 8), (0, 3, 1), (0, 3, 2), (0, 0, 9), (0, 3, 3), (0, 3, 4), (0, 0, 10),
        (0, 3, 5), (0, 2, 8), (0, 3, 6), (0, 2, 9), (0, 3, 7), (0, 0, 11), (0, 0, 0), (0, 2, 10),
        (0, 2, 0), (0, 2, 11), (0, 0, 1), (0, 2, 1), (0, 0, 2), (0, 2, 2), (0, 0, 3), (0, 2, 3),
        (0, 0, 4), (0, 1, 8), (0, 2, 4), (0, 0, 5), (0, 1, 9), (0, 2, 5), (0, 0, 6), (0, 1, 10),
        (0, 2, 6), (0, 3, 8), (0, 0, 7), (0, 1, 11), (0, 2, 7), (0, 3, 9), (0, 3, 10), (0, 3, 11),
    ),
    (False, False, 2): (
        (1, 0, 8), (1, 0, 9), (1, 0, 10), (1, 0, 11), (0, 2, 7), (0, 2, 8), (0, 2, 9), (0, 2, 0),
        (0, 2, 10), (0, 2, 11), (0, 2, 1), (0, 0, 7), (0, 0, 8), (0, 2, 2), (0, 0, 9), (0, 0, 10),
        (0, 2, 3), (0, 1, 7), (0, 3, 7), (0, 3, 0), (0, 0, 11), (0, 2, 4), (0, 3, 8), (0, 0, 0),
        (0, 1, 8), (0, 3, 1), (0, 3, 9), (0, 2, 5), (0, 3, 10), (0, 0, 1), (0, 1, 9), (0, 3, 2),
        (0, 3, 11), (0, 2, 6), (0, 1, 10), (0, 0, 2), (0, 1, 11), (0, 3, 3), (0, 0, 3), (0, 3, 4),
        (0, 0, 4), (0, 3, 5), (0, 0, 5), (0, 3, 6), (0, 0, 6), (0, 1, 0), (0, 1, 1), (0, 1, 2),
        (0, 1, 3), (0, 1, 4), (0, 1, 5), (0, 1, 6),
    ),
    (False, False, 3): (
        (1, 0, 8), (1, 1, 8), (1, 0, 9), (1, 1, 9), (1, 0, 10), (1, 1, 10), (1, 0, 11), (1, 1, 11),
        (0, 3, 0), (0, 3, 1), (0, 3, 2), (0, 3, 3), (0, 3, 4), (0, 3, 5), (0, 3, 6), (0, 3, 7),
        (0, 0, 0), (0, 2, 8), (0, 0, 1), (0, 0, 2), (0, 2, 9), (0, 0, 3), (0, 0, 8), (0, 0, 4),
        (0, 2, 10), (0, 0, 5), (0, 0, 9), (0, 0, 6), (0, 2, 11), (0, 2, 0), (0, 0, 10), (0, 0, 7),
        (0, 1, 0), (0, 0, 11), (0, 2, 1), (0, 1, 1), (0, 2, 2), (0, 1, 2), (0, 2, 3), (0, 1, 3),
        (0, 2, 4), (0, 3, 8), (0, 1, 4), (0, 2, 5), (0, 3, 9), (0, 1, 5), (0, 2, 6), (0, 3, 10),
        (0, 1, 6), (0, 1, 8), (0, 2, 7), (0, 3, 11), (0, 1, 7), (0, 1, 9), (0, 1, 10), (0, 1, 11),
    ),
}


def for_sending(array):
    return jax.tree.map(lambda a: a.astype(jnp.bfloat16) if a.dtype == jnp.float32 else a, array)


def column_sums(data, row_part, col_weight, col_blocks):
    row_mixed = jnp.dot(
        row_part[None, :], data.astype(jnp.float32), precision=lax.Precision.HIGHEST
    )[0]
    return jnp.sum((row_mixed * col_weight).reshape(col_blocks, -1), axis=1)


def shards(weights, first_moment, second_moment, row_weight, col_weight):
    dp_count = lax.axis_size("dp")
    pipe_count = lax.axis_size("pipe")
    tensor_count = lax.axis_size("tensor")
    shard_rows, width = weights.shape
    dp_section = dp_count // pipe_count
    tile_shards = dp_count // tensor_count
    piece_cols = width // dp_count
    tile_rows = shard_rows * dp_count
    col_blocks = width // CHECK_COLS
    factor = float(tile_rows * CHECK_COLS) ** (-0.5)
    sources = (weights, first_moment, second_moment)
    exchanged = (
        lax.all_to_all(sources[0], "dp", split_axis=1, concat_axis=0, tiled=True),
        lax.all_to_all(sources[1], "dp", split_axis=1, concat_axis=0, tiled=True),
        lax.all_to_all(sources[2], "dp", split_axis=1, concat_axis=0, tiled=True),
    )
    grouped = tuple(
        (item.reshape(pipe_count, dp_section, shard_rows, piece_cols) for item in exchanged)
    )
    sectioned = jax.tree.map(
        lambda part, own: part.astype(own.dtype),
        lax.all_to_all(for_sending(grouped), "pipe", split_axis=0, concat_axis=2, tiled=True),
        grouped,
    )
    routed = tuple(
        (item.reshape(tensor_count, tile_shards, 1, shard_rows, piece_cols) for item in sectioned)
    )
    arrived = jax.tree.map(
        lambda part, own: part.astype(own.dtype),
        lax.all_to_all(for_sending(routed), "tensor", split_axis=0, concat_axis=2, tiled=True),
        routed,
    )
    flat_pieces = tuple((item.reshape(tile_rows, piece_cols) for item in arrived))
    tiles = jax.tree.map(
        lambda part, own: part.astype(own.dtype),
        lax.all_gather(for_sending(flat_pieces), "dp", axis=1, tiled=True),
        flat_pieces,
    )
    tensor_pos = lax.axis_index("tensor")
    flat_index = (
        lax.axis_index("dp") * pipe_count + lax.axis_index("pipe")
    ) * tensor_count + tensor_pos
    in_section = flat_index % (dp_count * tensor_count)
    section_of = flat_index // (dp_count * tensor_count)
    tile_of = in_section // dp_count
    row_part = lax.dynamic_slice_in_dim(row_weight, in_section * shard_rows, shard_rows)
    partial_value = jnp.stack(
        [column_sums(item, row_part, col_weight, col_blocks) for item in sources]
    )
    section_hit = (jnp.arange(pipe_count) == section_of).astype(jnp.float32)
    tile_hit = (jnp.arange(tensor_count) == tile_of).astype(jnp.float32)
    spread = (
        partial_value[:, None, None, :]
        * section_hit[None, :, None, None]
        * tile_hit[None, None, :, None]
    )
    summed = lax.psum(spread, ("dp", "pipe", "tensor"))
    checks = (
        lax.dynamic_slice(summed, (0, lax.axis_index("pipe"), tensor_pos, 0), (3, 1, 1, col_blocks))
        * factor
    )
    return (tiles[0], tiles[1], tiles[2], checks)


def remote(src, dst, send_sem, recv_sem, where):
    return pltpu.make_async_remote_copy(
        src_ref=src,
        dst_ref=dst,
        send_sem=send_sem,
        recv_sem=recv_sem,
        device_id=where,
        device_id_type=pl.DeviceIdType.MESH,
    )


def route(
    count,
    w_ref,
    m_ref,
    v_ref,
    own,
    src,
    crossed,
    transit,
    load_sem,
    cross_send,
    cross_recv,
    z_send,
    relay_send,
    own_recv,
    transit_recv,
    hop_send,
    core_send,
):
    dp, y, z = lax.axis_index("dp"), lax.axis_index("pipe"), lax.axis_index("tensor")
    x, core = dp // 2, dp % 2
    hub = z // 2
    diag = x == y
    mine = 2 * core + y
    rows = w_ref.shape[0]
    edges = [rows // 8 * h // SPLIT * 8 for h in range(SPLIT)] + [rows]
    cuts = [pl.ds(low, high - low) for low, high in zip(edges, edges[1:])]
    units = range(3 * SPLIT)

    def unit(ref, u):
        return ref.at[u // SPLIT, cuts[u % SPLIT]]

    def at(to_x, to_y, to_core, to_z=None):
        return {"dp": to_x * 2 + to_core, "pipe": to_y, "tensor": z if to_z is None else to_z}

    core_to = at(x, y, 1 - core)
    x_to = at(1 - x, y, 1 - core)
    y_to = at(x, 1 - y, 1 - core)
    both_to = at(1 - x, 1 - y, 1 - core)

    ins = (w_ref, m_ref, v_ref)
    loads = [pltpu.make_async_copy(ins[a], src.at[a], load_sem.at[a]) for a in range(3)]
    for load in loads:
        load.start()

    barrier = pltpu.get_barrier_semaphore()
    partners = [core_to, x_to, y_to, both_to, at(x, 1 - y, core)]
    for step in range(1, count):
        partners += [at(x, y, c, (z + step) % count) for c in (core, 1 - core)]
    for where in partners:
        pl.semaphore_signal(barrier, inc=1, device_id=where, device_id_type=pl.DeviceIdType.MESH)
    pl.semaphore_wait(barrier, len(partners))
    for load in loads:
        load.wait()

    def start(copy):
        copy.start()

    def sent(copy):
        copy.wait_send()

    def home(on_diag, k, u):
        if on_diag:
            return unit(own.at[k], u), own_recv.at[k, u]
        return unit(transit.at[k], u), transit_recv.at[k, u]

    def cross(on_diag, u, act):
        slot, sem = home(not on_diag, z, u)
        relay = unit(crossed.at[core], u)

        @pl.when(mine == z)
        def _():
            act(remote(unit(src, u), slot, cross_send.at[u], sem, at(x, 1 - y, hub)))

        @pl.when(mine != z)
        def _():
            act(remote(unit(src, u), relay, cross_send.at[u], cross_recv.at[core, u], at(x, 1 - y, 1 - hub)))

    def along(on_diag, u, act):
        slot, sem = home(on_diag, z, u)

        @pl.when(mine != z)
        def _():
            act(remote(unit(src, u), slot, z_send.at[u], sem, at(x, y, core, mine)))

        if act is start:

            @pl.when(mine == z)
            def _():
                pltpu.make_async_copy(unit(src, u), slot, sem).start()

    def relay(on_diag, c, u):
        slot, sem = home(on_diag, z, u)
        return remote(unit(crossed.at[c], u), slot, relay_send.at[c, u], sem, at(x, y, c, 2 * c + 1 - y))

    def landed(slot, sem):
        pltpu.make_async_copy(slot, slot, sem).wait()

    def arrive(k, u):
        landed(*home(True, k, u))

    def across(k, u):
        slot, sem = home(True, k, u)
        return remote(slot, slot, core_send.at[k, u], sem, core_to)

    def forward_x(k, u):
        slot, sem = home(True, k, u)
        return remote(slot, slot, hop_send.at[0, k, u], sem, x_to)

    def forward_off(n, k, u):
        slot, sem = home(True, k, u)
        return remote(unit(transit.at[k], u), slot, hop_send.at[n, k, u], sem, (y_to, both_to)[n])

    def flip(low, high):
        return low + x * (high - 2 * low)

    for on_diag in (True, False):

        @pl.when(diag == on_diag)
        def _():
            limit = OWN_UNITS if on_diag else OFF_UNITS
            for u in units:
                if (u < limit) != on_diag:
                    cross(on_diag, u, start)
            for u in units:
                if (u < limit) == on_diag:
                    along(on_diag, u, start)

    place = flip(z, count - 1)

    def run(on_diag, is_hub, zr):
        limit = OFF_UNITS if zr % 2 else OWN_UNITS
        for kind, kr, u in ORDER[on_diag, is_hub, zr]:
            if kind:
                c = flip(kr, 1)
                landed(unit(crossed.at[c], u), cross_recv.at[c, u])
                relay(on_diag, c, u).start()
                continue
            k = flip(kr, count - 1)
            if is_hub and not on_diag:
                landed(*home(False, k, u))
                forward_off(0, k, u).start()
                forward_off(1, k, u).start()
            else:
                arrive(k, u)
                if is_hub:
                    forward_x(k, u).start()
                across(k, u).start()

        @pl.loop(0, count)
        def _(kr):
            k = flip(kr, count - 1)
            for u in units:
                here = is_hub == (on_diag and u < limit)
                if is_hub and not on_diag:
                    arrive(k, u)
                    if u >= limit:
                        forward_off(0, k, u).wait_send()
                        forward_off(1, k, u).wait_send()
                elif here:
                    if is_hub:
                        forward_x(k, u).wait_send()
                    across(k, u).wait_send()
                else:
                    arrive(k, u)

        if not is_hub:
            for cr in (0, 1):
                for u in units:
                    odd = OFF_UNITS if on_diag else OWN_UNITS
                    if 2 * cr + on_diag != zr and (u < odd) == on_diag:
                        relay(on_diag, flip(cr, 1), u).wait_send()

    for on_diag in (True, False):
        for is_hub in (True, False):
            for zr in range(count):

                @pl.when((diag == on_diag) & ((hub == core) == is_hub) & (place == zr))
                def _():
                    run(on_diag, is_hub, zr)

    for on_diag in (True, False):

        @pl.when(diag == on_diag)
        def _():
            limit = OWN_UNITS if on_diag else OFF_UNITS
            for u in units:
                if (u < limit) == on_diag:
                    along(on_diag, u, sent)
                else:
                    cross(on_diag, u, sent)


def finish(count, own, row_ref, col_ref, out0, out1, out2, check_ref, acc, out_sem):
    rows, width = own.shape[2:]
    outs = (out0, out1, out2)
    leaving = [
        pltpu.make_async_copy(own.at[k, a], outs[a].at[k], out_sem.at[a, k])
        for a in range(3)
        for k in range(count)
    ]
    for copy in leaving:
        copy.start()
    acc[...] = jnp.zeros_like(acc)
    for k in range(count):
        first = (lax.axis_index("tensor") * count + k) * rows
        everyone = jnp.broadcast_to(row_ref[...].reshape(1, width), (8, width))
        part = pltpu.roll(everyone, (width - first) % width, 1)[:, :rows]
        high = part.astype(jnp.bfloat16).astype(jnp.float32)
        middle = (part - high).astype(jnp.bfloat16).astype(jnp.float32)
        low = part - high - middle
        line = lax.broadcasted_iota(jnp.int32, (8, rows), 0)
        terms = jnp.where(
            line == 0, high, jnp.where(line == 1, middle, jnp.where(line == 2, low, 0.0))
        )
        terms = terms.astype(jnp.bfloat16)
        for a in range(3):
            acc[a] += jnp.dot(terms, own[k, a], preferred_element_type=jnp.float32)

    factor = float(rows * count * CHECK_COLS) ** (-0.5)
    blocks = width // CHECK_COLS
    weight = col_ref[...].reshape(1, width)
    for a in range(3):
        mixed = jnp.sum(acc[a], axis=0, keepdims=True) * weight
        lane = lax.broadcasted_iota(jnp.int32, (1, blocks), 1)
        line = jnp.zeros((1, blocks), jnp.float32)
        for e in range(blocks):
            part = jnp.sum(mixed[:, e * CHECK_COLS : (e + 1) * CHECK_COLS], axis=1, keepdims=True)
            line = jnp.where(lane == e, part, line)
        check_ref[a, 0] = line * factor
    for copy in leaving:
        copy.wait()


def routed(weights, first_moment, second_moment, row_weight, col_weight):
    count = lax.axis_size("dp")
    rows, width = weights.shape
    blocks = width // CHECK_COLS
    vmem = pl.BlockSpec(memory_space=pltpu.VMEM)
    anywhere = pl.BlockSpec(memory_space=pl.ANY)
    tile = jax.ShapeDtypeStruct((count, rows, width), weights.dtype)
    dma = pltpu.SemaphoreType.DMA
    own = pl.pallas_call(
        functools.partial(route, count),
        out_shape=pltpu.VMEM((count, 3, rows, width), weights.dtype),
        in_specs=[anywhere] * 3,
        out_specs=vmem,
        scratch_shapes=[
            pltpu.VMEM((3, rows, width), weights.dtype),
            pltpu.VMEM((2, 3, rows, width), weights.dtype),
            pltpu.VMEM((count, 3, rows, width), weights.dtype),
            dma((3,)),
            dma((3 * SPLIT,)),
            dma((2, 3 * SPLIT)),
            dma((3 * SPLIT,)),
            dma((2, 3 * SPLIT)),
            dma((count, 3 * SPLIT)),
            dma((count, 3 * SPLIT)),
            dma((2, count, 3 * SPLIT)),
            dma((count, 3 * SPLIT)),
        ],
        compiler_params=pltpu.CompilerParams(
            collective_id=0, has_side_effects=True
        ),
    )(weights, first_moment, second_moment)
    out = pl.pallas_call(
        functools.partial(finish, count),
        out_shape=(tile, tile, tile, jax.ShapeDtypeStruct((3, 1, 1, blocks), jnp.float32)),
        in_specs=[vmem, vmem, vmem],
        out_specs=(anywhere, anywhere, anywhere, vmem),
        scratch_shapes=[pltpu.VMEM((3, 8, width), jnp.float32), dma((3, count))],
        compiler_params=pltpu.CompilerParams(vmem_limit_bytes=16 * 1024 * 1024),
    )(own, row_weight, col_weight)
    return tuple(item.reshape(count * rows, width) for item in out[:3]) + (out[3],)


def solution(mesh):
    dp_count, pipe_count, tensor_count = (mesh.shape[a] for a in ("dp", "pipe", "tensor"))
    square = dp_count == tensor_count == 2 * pipe_count and pipe_count == 2
    return jax.shard_map(
        routed if square else shards,
        mesh=mesh,
        in_specs=(
            P(("dp", "pipe", "tensor"), None),
            P(("dp", "pipe", "tensor"), None),
            P(("dp", "pipe", "tensor"), None),
            P(),
            P(),
        ),
        out_specs=(
            P(("pipe", "tensor"), None),
            P(("pipe", "tensor"), None),
            P(("pipe", "tensor"), None),
            P(None, "pipe", "tensor", None),
        ),
        check_vma=False,
    )
```
